256 devices in a mesh: rows: 16 (over y_hi, z), pairs: 16 (over x, y_lo, core).
Axes of the slice: x: 4, y: 4 (y_hi: 2, y_lo: 2; y = y_hi * 2 + y_lo), z: 8, core: 2. Of those that a mesh axis runs over, the one named last changes fastest.
Arguments:
- matrix: float32 [32768, 8192], P('rows', 'pairs'), may hold values from -40 to 40
Outputs:
- rotated: float32 [32768, 8192], P('rows', 'pairs')
The draws below stay inside these ranges and needn't reach their ends.
All inputs are finite; a program needn't handle non-finite values.
Results may differ from the reference program's by a relative error of at most 0.0001.
Values sent between devices are 32-bit elements; how exact they have to be, the bound alone decides.
No kernel may reach another device: no remote copies, remote signals or barrier semaphores. Data moves between devices by JAX's collectives and lax.ppermute only.
A program may use at most 64 MiB of HBM per device.

```python
import jax
import jax.numpy as jnp
from jax import lax

B = 256
STEPS = 2
PAIRS = 16
ROWS = 32768
COLS = 8192


def draw_matrix(key, part):
    keys = jax.random.split(jax.random.fold_in(key, 17), 4)
    independent = jax.random.normal(keys[0], (ROWS, COLS), jnp.float32)
    shared_scale = 0.05
    factors = jax.random.normal(keys[1], (ROWS, 64), jnp.float32)
    loadings = jax.random.normal(keys[2], (64, COLS), jnp.float32) * shared_scale
    shared = jnp.dot(factors, loadings, preferred_element_type=jnp.float32)
    col_scale = jnp.exp(jax.random.uniform(keys[3], (1, COLS), jnp.float32, jnp.log(0.3), jnp.log(3.0)))
    values = (independent + shared) * col_scale
    return jnp.clip(values, -40.0, 40.0).astype(jnp.float32)


def setup_inputs(seed: int = 0) -> dict:
    key_list = jax.random.split(jax.random.key(seed), 2)
    matrix = draw_matrix(jax.random.fold_in(key_list[1], 71), 0)
    return dict(matrix=matrix)


def spd_solve(system, right_side):
    factor = jnp.linalg.cholesky(system)
    middle = lax.linalg.triangular_solve(factor, right_side, left_side=True, lower=True)
    return lax.linalg.triangular_solve(factor, middle, left_side=True, lower=True, transpose_a=True)

def cayley_rotation(cross_block, norms_first, norms_second, rows_all):
    precise = lax.Precision.HIGHEST
    block_cols = cross_block.shape[0]
    scale_first = lax.rsqrt(norms_first / rows_all + 1e-06)
    scale_second = lax.rsqrt(norms_second / rows_all + 1e-06)
    coupling = 0.5 * cross_block * scale_first[:, None] * scale_second[None, :] / rows_all
    identity = jnp.eye(block_cols, dtype=jnp.float32)
    first_system = identity + jnp.dot(coupling.astype(jnp.float32), coupling.T.astype(jnp.float32), precision=precise, preferred_element_type=jnp.float32)
    first_sol = spd_solve(first_system, jnp.concatenate([identity, coupling], axis=1))
    lower_sol = jnp.dot(coupling.T.astype(jnp.float32), first_sol.astype(jnp.float32), precision=precise, preferred_element_type=jnp.float32)
    upper_rows = jnp.concatenate([2.0 * first_sol[:, :block_cols] - identity, 2.0 * first_sol[:, block_cols:]], axis=1)
    lower_rows = jnp.concatenate([-2.0 * lower_sol[:, :block_cols], identity - 2.0 * lower_sol[:, block_cols:]], axis=1)
    return jnp.concatenate([upper_rows, lower_rows], axis=0)

def reference(matrix):
    precise = lax.Precision.HIGHEST
    grouped = matrix.reshape(ROWS, PAIRS, 2, B)
    first_blocks = jnp.transpose(grouped[:, :, 0, :], (1, 0, 2))
    second_blocks = jnp.transpose(grouped[:, :, 1, :], (1, 0, 2))

    def turn_pair(pair_blocks):
        both = jnp.concatenate([pair_blocks[0], pair_blocks[1]], axis=1)
        gram_pair = lax.dot_general(both.astype(jnp.float32), both.astype(jnp.float32), (((0,), (0,)), ((), ())), precision=precise, preferred_element_type=jnp.float32)
        diag_all = jnp.diagonal(gram_pair)
        rotate = cayley_rotation(gram_pair[:B, B:], diag_all[:B], diag_all[B:], ROWS)
        turned = jnp.dot(both.astype(jnp.float32), rotate.astype(jnp.float32), precision=precise, preferred_element_type=jnp.float32)
        return (turned[:, :B], turned[:, B:])
    for turn_index in range(STEPS):
        first_blocks, second_blocks = lax.map(turn_pair, (first_blocks, second_blocks))
        next_first = jnp.concatenate([first_blocks[:1], second_blocks[:1], first_blocks[1:-1]], axis=0)
        second_blocks = jnp.concatenate([second_blocks[1:], first_blocks[-1:]], axis=0)
        first_blocks = next_first
    stacked = jnp.stack([first_blocks, second_blocks], axis=2)
    return jnp.transpose(stacked, (1, 0, 2, 3)).reshape(ROWS, COLS)
```

```python
import jax
import jax.numpy as jnp
from jax import lax
from jax.experimental import pallas as pl
from jax.experimental.pallas import tpu as pltpu
from jax.sharding import PartitionSpec as P

F32, BF16 = jnp.float32, jnp.bfloat16
TAIL = 8
LANES = 128


def halves(x):
    high = x.astype(BF16)
    return high, (x - high.astype(F32)).astype(BF16)


def product(a, b, dims=((1,), (0,))):
    return lax.dot_general(a, b, (dims, ((), ())), preferred_element_type=F32)


def three_products(a, b, dims=((1,), (0,))):
    (a_high, a_low), (b_high, b_low) = halves(a), halves(b)
    return product(a_high, b_high, dims) + (product(a_high, b_low, dims) + product(a_low, b_high, dims))


def full_product(a, b, dims=((1,), (0,))):
    return lax.dot_general(
        a, b, (dims, ((), ())), precision=lax.Precision.HIGHEST, preferred_element_type=F32
    )


def gram(left, left_at, right, right_at, peers, cols, block=512):
    per, wide = cols // peers, cols // LANES

    def kernel(left_ref, right_ref, out_ref, acc_ref, norms_ref):
        step = pl.program_id(0)

        @pl.when(step == 0)
        def _():
            acc_ref[...] = jnp.zeros_like(acc_ref)
            norms_ref[...] = jnp.zeros_like(norms_ref)

        a, b = left_ref[...], right_ref[...]
        acc_ref[...] += three_products(a, b, ((0,), (0,)))
        norms_ref[:, :cols] += jnp.sum((a * a).reshape(block // 8, 8, cols), axis=0)
        norms_ref[:, cols:] += jnp.sum((b * b).reshape(block // 8, 8, cols), axis=0)

        @pl.when(step == pl.num_programs(0) - 1)
        def _():
            total = jnp.sum(norms_ref[...], axis=0, keepdims=True)
            lines = [total[:, LANES * q : LANES * (q + 1)] for q in range(2 * wide)]
            tail = jnp.concatenate([*lines, jnp.zeros((TAIL - 2 * wide, LANES), F32)], axis=0)
            for peer in range(peers):
                rows = acc_ref[peer * per : (peer + 1) * per, :]
                for q in range(wide):
                    out_ref[peer, q * per : (q + 1) * per, :] = rows[:, LANES * q : LANES * (q + 1)]
                out_ref[peer, wide * per :, :] = tail

    shape = (peers, wide * per + TAIL, LANES)
    return pl.pallas_call(
        kernel,
        grid=(left.shape[0] // block,),
        in_specs=[
            pl.BlockSpec((block, cols), lambda i: (i, left_at)),
            pl.BlockSpec((block, cols), lambda i: (i, right_at)),
        ],
        out_specs=pl.BlockSpec(shape, lambda i: (0, 0, 0)),
        out_shape=jax.ShapeDtypeStruct(shape, F32),
        scratch_shapes=[pltpu.VMEM((cols, cols), F32), pltpu.VMEM((8, 2 * cols), F32)],
        name="gram",
    )(left, right)


def slab_sum(slabs, cols):
    peers = slabs.shape[0]
    per, wide = cols // peers, cols // LANES

    def kernel(in_ref, out_ref):
        total = in_ref[0]
        for peer in range(1, peers):
            total = total + in_ref[peer]
        rows = [total[q * per : (q + 1) * per] for q in range(wide)]
        out_ref[:per] = jnp.concatenate(rows, axis=1)
        tail = total[wide * per :]
        for side in range(2):
            lines = [tail[side * wide + q : side * wide + q + 1] for q in range(wide)]
            out_ref[per + side : per + side + 1] = jnp.concatenate(lines, axis=1)
        out_ref[per + 2 :] = jnp.zeros((TAIL - 2, cols), F32)

    return pl.pallas_call(
        kernel, out_shape=jax.ShapeDtypeStruct((per + TAIL, cols), F32), name="slab_sum"
    )(slabs)


def cayley(cross, norms, sign, rows_all, power_ref, inverse_ref):
    cols = cross.shape[0]
    scale_left = lax.rsqrt(norms[0:1] / rows_all + 1e-06)
    scale_right = lax.rsqrt(norms[1:2] / rows_all + 1e-06)
    row_at = lax.broadcasted_iota(jnp.int32, (cols, cols), 0)
    col_at = lax.broadcasted_iota(jnp.int32, (cols, cols), 1)
    diagonal = row_at == col_at
    identity = jnp.where(diagonal, 1.0, 0.0).astype(F32)
    spread = jnp.where(diagonal, jnp.broadcast_to(scale_left, (cols, cols)), 0.0)
    scale_left = jnp.sum(spread, axis=1, keepdims=True)
    coupling = (0.5 * sign) * cross * scale_left * scale_right / rows_all
    system = identity + full_product(coupling, coupling, ((1,), (1,)))
    bound = jnp.max(jnp.sum(jnp.abs(system), axis=0, keepdims=True))
    factor = 2.0 / (1.0 + bound)
    power = identity - factor * system
    inverse_ref[...] = factor * (identity + power)
    power_ref[...] = power
    ratio = (bound - 1.0) / (bound + 1.0)

    def more(carry):
        left, count = carry
        return (left > 1e-3) & (count < 40)

    def double(carry):
        left, count = carry
        before = power_ref[...]
        squared = three_products(before, before)
        power_ref[...] = squared
        inverse = inverse_ref[...]
        inverse_ref[...] = inverse + three_products(inverse, squared)
        return left * left, count + 1

    lax.while_loop(more, double, (ratio * ratio, jnp.int32(0)))

    def newton(_, carry):
        inverse = inverse_ref[...]
        inverse_ref[...] = inverse + full_product(inverse, identity - full_product(system, inverse))
        return carry

    lax.fori_loop(0, jnp.where(bound < 8.0, 1, 3), newton, 0)
    inverse = inverse_ref[...]
    upper = full_product(inverse, coupling)
    lower = full_product(coupling, upper, ((0,), (0,)))
    return 2.0 * inverse - identity, 2.0 * upper, -2.0 * upper.T, identity - 2.0 * lower


def store_halves(high_ref, low_ref, at_row, at_col, value):
    rows, cols = value.shape
    high, low = halves(value)
    high_ref[at_row : at_row + rows, at_col : at_col + cols] = high
    low_ref[at_row : at_row + rows, at_col : at_col + cols] = low


def step_one_matrices(gathered, norms, swap, rows_all):
    cols = gathered.shape[2]

    def kernel(swap_ref, cross_ref, norms_ref, high_ref, low_ref, power_ref, inverse_ref):
        cross = cross_ref[...].reshape(cols, cols)
        blocks = cayley(cross, norms_ref[...], 1.0, rows_all, power_ref, inverse_ref)
        turned = swap_ref[0] != 0
        for line in range(2):
            near, far = blocks[2 * line], blocks[2 * line + 1]
            store_halves(high_ref, low_ref, line * cols, 0, jnp.where(turned, far, near))
            store_halves(high_ref, low_ref, line * cols, cols, jnp.where(turned, near, far))

    out = jax.ShapeDtypeStruct((2 * cols, 2 * cols), BF16)
    vmem = pl.BlockSpec(memory_space=pltpu.VMEM)
    return pl.pallas_call(
        kernel,
        in_specs=[pl.BlockSpec(memory_space=pltpu.SMEM), vmem, vmem],
        out_shape=(out, out),
        scratch_shapes=[pltpu.VMEM((cols, cols), F32)] * 2,
        name="cayley_one",
    )(swap, gathered, norms)


def step_two_matrices(gathered, norms, other_norms, marks, rows_all):
    peers, both, cols = gathered.shape
    per = both // 2

    def kernel(marks_ref, cross_ref, norms_ref, other_ref, *refs):
        outs, (power_ref, inverse_ref) = refs[:4], refs[4:]
        for edge in range(2):
            cross = cross_ref[:, edge * per : (edge + 1) * per, :].reshape(cols, cols)
            sign = jnp.where(marks_ref[2 * edge] != 0, 1.0, -1.0).astype(F32)
            lines = (norms_ref, other_ref)[edge][...]
            blocks = cayley(cross, lines, sign, rows_all, power_ref, inverse_ref)
            moved_role = marks_ref[2 * edge + 1] != 0
            for line in range(2):
                value = jnp.where(moved_role, blocks[2 * line], blocks[2 * line + 1])
                store_halves(outs[2 * edge], outs[2 * edge + 1], line * cols, 0, value)

    out = jax.ShapeDtypeStruct((2 * cols, cols), BF16)
    vmem = pl.BlockSpec(memory_space=pltpu.VMEM)
    return pl.pallas_call(
        kernel,
        in_specs=[pl.BlockSpec(memory_space=pltpu.SMEM), vmem, vmem, vmem],
        out_shape=(out,) * 4,
        scratch_shapes=[pltpu.VMEM((cols, cols), F32)] * 2,
        name="cayley_two",
    )(marks, gathered, norms, other_norms)


def rotate(both, high, low, block=256):
    rows, width = both.shape
    cols = width // 2

    def kernel(x_ref, high_ref, low_ref, first_ref, second_ref):
        x_high, x_low = halves(x_ref[...])
        turned = product(x_high, high_ref[...]) + (
            product(x_high, low_ref[...]) + product(x_low, high_ref[...])
        )
        first_ref[...] = turned[:, :cols]
        second_ref[...] = turned[:, cols:]

    fixed = pl.BlockSpec((width, width), lambda i: (0, 0))
    half = pl.BlockSpec((block, cols), lambda i: (i, 0))
    return pl.pallas_call(
        kernel,
        grid=(rows // block,),
        in_specs=[pl.BlockSpec((block, width), lambda i: (i, 0)), fixed, fixed],
        out_specs=(half, half),
        out_shape=(jax.ShapeDtypeStruct((rows, cols), F32),) * 2,
        name="rotate",
    )(both, high, low)


def combine(at, left, right, high, low, before=None, block=256):
    rows, cols = left.shape

    def kernel(at_ref, left_ref, right_ref, high_ref, low_ref, *refs):
        out_ref = refs[-1]
        total = jnp.zeros((block, cols), F32)
        for line, ref in enumerate((left_ref, right_ref)):
            x_high, x_low = halves(ref[...])
            m_high = high_ref[line * cols : (line + 1) * cols, :]
            m_low = low_ref[line * cols : (line + 1) * cols, :]
            total += product(x_high, m_high) + (product(x_high, m_low) + product(x_low, m_high))
        out_ref[...] = total

    data = pl.BlockSpec((block, cols), lambda i, at_ref: (i, 0))
    fixed = pl.BlockSpec((2 * cols, cols), lambda i, at_ref: (0, 0))
    operands = [at, left, right, high, low]
    in_specs = [data, data, fixed, fixed]
    aliases = {}
    if before is not None:
        operands.append(before)
        in_specs.append(pl.BlockSpec(memory_space=pl.ANY))
        aliases = {len(operands) - 1: 0}
    return pl.pallas_call(
        kernel,
        grid_spec=pltpu.PrefetchScalarGridSpec(
            num_scalar_prefetch=1,
            grid=(rows // block,),
            in_specs=in_specs,
            out_specs=pl.BlockSpec((block, cols), lambda i, at_ref: (i, at_ref[0])),
        ),
        out_shape=jax.ShapeDtypeStruct((rows, 2 * cols), F32),
        input_output_aliases=aliases,
        name="combine",
    )(*operands)


def exchanged(blocks):
    return lax.all_to_all(blocks, "rows", 0, 0, tiled=True)


def shards(matrix):
    cols = matrix.shape[1] // 2
    peers = lax.axis_size("rows")
    rows_all = matrix.shape[0] * peers
    per = cols // peers
    position = lax.axis_index("pairs")
    size = lax.axis_size("pairs")
    ring = [*range(0, size, 2), *range(size - 1, 0, -2)]
    clockwise = [(ring[i], ring[(i + 1) % size]) for i in range(size)]
    back = [(b, a) for a, b in clockwise]
    even = position % 2 == 0

    slabs = exchanged(gram(matrix, 0, matrix, 1, peers, cols))
    mine = slab_sum(slabs, cols)
    gathered = exchanged(jnp.broadcast_to(mine[:per], (peers, per, cols)))
    swap = jnp.where(even & (position > 0), 0, 1).astype(jnp.int32)[None]
    high, low = step_one_matrices(gathered, mine[per:], swap, float(rows_all))
    onward, kept = rotate(matrix, high, low)

    arrived = lax.ppermute(onward, "pairs", clockwise)
    kept_late, arrived = lax.optimization_barrier((kept, arrived))
    returned = lax.ppermute(kept_late, "pairs", back)
    slabs = exchanged(gram(arrived, 0, kept, 0, peers, cols))
    mine = slab_sum(slabs, cols)
    other = lax.ppermute(mine, "pairs", back)
    pair = jnp.concatenate([mine[:per], other[:per]], axis=0)
    gathered = exchanged(jnp.broadcast_to(pair, (peers, 2 * per, cols)))
    marks = jnp.stack(
        [
            (even & (position > 0)) | (position == size - 1),
            position != 0,
            even,
            position == 1,
        ]
    ).astype(jnp.int32)
    matrices = step_two_matrices(gathered, mine[per:], other[per:], marks, float(rows_all))
    in_first = jnp.where(even, 0, 1).astype(jnp.int32)[None]
    half_done = combine(in_first, arrived, kept, *matrices[:2])
    return combine(1 - in_first, onward, returned, *matrices[2:], before=half_done)


def solution(mesh):
    return jax.shard_map(
        shards,
        mesh=mesh,
        in_specs=(P("rows", "pairs"),),
        out_specs=P("rows", "pairs"),
        check_vma=False,
    )
```

```python
import jax
import jax.numpy as jnp
from jax import lax
from jax.experimental import pallas as pl
from jax.experimental.pallas import tpu as pltpu
from jax.sharding import PartitionSpec as P


F32, BF16 = jnp.float32, jnp.bfloat16
TAIL = 8
LANES = 128


def halves(x):
    high = x.astype(BF16)
    return high, (x - high.astype(F32)).astype(BF16)


def product(a, b, dims=((1,), (0,))):
    return lax.dot_general(a, b, (dims, ((), ())), preferred_element_type=F32)


def three_products(a, b, dims=((1,), (0,))):
    (a_high, a_low), (b_high, b_low) = halves(a), halves(b)
    return product(a_high, b_high, dims) + (product(a_high, b_low, dims) + product(a_low, b_high, dims))


def full_product(a, b, dims=((1,), (0,))):
    return lax.dot_general(
        a, b, (dims, ((), ())), precision=lax.Precision.HIGHEST, preferred_element_type=F32
    )


def gram_parts(lefts, rights, cols, before=()):
    pieces = len(lefts)

    def kernel(*refs):
        ins, (acc_ref, norms_ref) = refs[:-2], refs[-2:]
        acc = norms = None
        for a_ref, b_ref in zip(ins[:pieces], ins[pieces : 2 * pieces]):
            a, b = a_ref[...], b_ref[...]
            part = three_products(a, b, ((0,), (0,)))
            squares = jnp.concatenate([a * a, b * b], axis=1)
            squares = jnp.sum(squares.reshape(a.shape[0] // 8, 8, 2 * cols), axis=0)
            acc = part if acc is None else acc + part
            norms = squares if norms is None else norms + squares
        if before:
            acc, norms = acc + ins[-2][...], norms + ins[-1][...]
        acc_ref[...] = acc
        norms_ref[...] = norms

    return pl.pallas_call(
        kernel,
        out_shape=(
            jax.ShapeDtypeStruct((cols, cols), F32),
            jax.ShapeDtypeStruct((8, 2 * cols), F32),
        ),
        name="gram_parts",
    )(*lefts, *rights, *before)


def store_slabs(out_ref, acc_ref, norms, peers, cols):
    per, wide = cols // peers, cols // LANES
    total = jnp.sum(norms, axis=0, keepdims=True)
    lines = [total[:, LANES * q : LANES * (q + 1)] for q in range(2 * wide)]
    tail = jnp.concatenate([*lines, jnp.zeros((TAIL - 2 * wide, LANES), F32)], axis=0)
    for peer in range(peers):
        rows = acc_ref[peer * per : (peer + 1) * per, :]
        for q in range(wide):
            out_ref[peer, q * per : (q + 1) * per, :] = rows[:, LANES * q : LANES * (q + 1)]
        out_ref[peer, wide * per :, :] = tail


def gram(left, left_at, right, right_at, rows, peers, cols, before=(), block=512):
    per, wide = cols // peers, cols // LANES

    def kernel(left_ref, right_ref, *refs):
        out_ref, acc_ref, norms_ref = refs[-3:]
        step = pl.program_id(0)

        @pl.when(step == 0)
        def _():
            if before:
                acc_ref[...] = refs[0][...]
                norms_ref[...] = refs[1][...]
            else:
                acc_ref[...] = jnp.zeros_like(acc_ref)
                norms_ref[...] = jnp.zeros_like(norms_ref)

        a, b = left_ref[...], right_ref[...]
        acc_ref[...] += three_products(a, b, ((0,), (0,)))
        norms_ref[:, :cols] += jnp.sum((a * a).reshape(block // 8, 8, cols), axis=0)
        norms_ref[:, cols:] += jnp.sum((b * b).reshape(block // 8, 8, cols), axis=0)

        @pl.when(step == pl.num_programs(0) - 1)
        def _():
            store_slabs(out_ref, acc_ref, norms_ref[...], peers, cols)

    shape = (peers, wide * per + TAIL, LANES)
    return pl.pallas_call(
        kernel,
        grid=(rows // block,),
        in_specs=[
            pl.BlockSpec((block, cols), lambda i: (i, left_at)),
            pl.BlockSpec((block, cols), lambda i: (i, right_at)),
            *[pl.BlockSpec(x.shape, lambda i: (0, 0)) for x in before],
        ],
        out_specs=pl.BlockSpec(shape, lambda i: (0, 0, 0)),
        out_shape=jax.ShapeDtypeStruct(shape, F32),
        scratch_shapes=[pltpu.VMEM((cols, cols), F32), pltpu.VMEM((8, 2 * cols), F32)],
        name="gram",
    )(left, right, *before)


def slab_sum(slabs, cols, spread):
    peers = slabs.shape[0]
    per, wide = cols // peers, cols // LANES

    def kernel(in_ref, out_ref, norms_ref):
        total = in_ref[0]
        for peer in range(1, peers):
            total = total + in_ref[peer]
        rows = jnp.concatenate([total[q * per : (q + 1) * per] for q in range(wide)], axis=1)
        if spread:
            for peer in range(peers):
                out_ref[peer] = rows
        else:
            out_ref[:per] = rows
        tail = total[wide * per :]
        norms = []
        for side in range(2):
            lines = [tail[side * wide + q : side * wide + q + 1] for q in range(wide)]
            norms.append(jnp.concatenate(lines, axis=1))
        norms = jnp.concatenate([*norms, jnp.zeros((TAIL - 2, cols), F32)], axis=0)
        norms_ref[...] = norms
        if not spread:
            out_ref[per:] = norms

    shape = (peers, per, cols) if spread else (per + TAIL, cols)
    return pl.pallas_call(
        kernel,
        out_shape=(jax.ShapeDtypeStruct(shape, F32), jax.ShapeDtypeStruct((TAIL, cols), F32)),
        name="slab_sum",
    )(slabs)


def paired(mine, other, partner, peers, per):
    cols = mine.shape[1]

    def kernel(mine_ref, other_ref, partner_ref, out_ref, norms_ref, other_norms_ref):
        sums = []
        for edge, ref in enumerate((mine_ref, other_ref)):
            begin = edge * (per + TAIL)
            sums.append(ref[...] + partner_ref[begin : begin + per + TAIL])
        for peer in range(peers):
            out_ref[peer, :per] = sums[0][:per]
            out_ref[peer, per:] = sums[1][:per]
        norms_ref[...] = sums[0][per:]
        other_norms_ref[...] = sums[1][per:]

    norms = jax.ShapeDtypeStruct((TAIL, cols), F32)
    return pl.pallas_call(
        kernel,
        out_shape=(jax.ShapeDtypeStruct((peers, 2 * per, cols), F32), norms, norms),
        name="paired",
    )(mine, other, partner)


def cayley(edges, rows_all, power_refs, inverse_refs):
    cols = edges[0][0].shape[0]
    row_at = lax.broadcasted_iota(jnp.int32, (cols, cols), 0)
    col_at = lax.broadcasted_iota(jnp.int32, (cols, cols), 1)
    diagonal = row_at == col_at
    identity = jnp.where(diagonal, 1.0, 0.0).astype(F32)
    couplings, systems, bounds = [], [], []
    for cross, norms, sign in edges:
        scale_left = lax.rsqrt(norms[0:1] / rows_all + 1e-06)
        scale_right = lax.rsqrt(norms[1:2] / rows_all + 1e-06)
        spread = jnp.where(diagonal, jnp.broadcast_to(scale_left, (cols, cols)), 0.0)
        scale_left = jnp.sum(spread, axis=1, keepdims=True)
        coupling = (0.5 * sign) * cross * scale_left * scale_right / rows_all
        couplings.append(coupling)
        systems.append(identity + full_product(coupling, coupling, ((1,), (1,))))
    for system, power_ref, inverse_ref in zip(systems, power_refs, inverse_refs):
        bound = jnp.max(jnp.sum(jnp.abs(system), axis=0, keepdims=True))
        factor = 2.0 / (1.0 + bound)
        power = identity - factor * system
        inverse_ref[...] = factor * (identity + power)
        power_ref[...] = power
        bounds.append(bound)
    largest = bounds[0] if len(bounds) == 1 else jnp.maximum(*bounds)
    ratio = (largest - 1.0) / (largest + 1.0)

    def more(carry):
        left, count = carry
        return (left > 1e-3) & (count < 40)

    def double(carry):
        left, count = carry
        squares = []
        for power_ref in power_refs:
            before = power_ref[...]
            squares.append(three_products(before, before))
        for squared, power_ref, inverse_ref in zip(squares, power_refs, inverse_refs):
            power_ref[...] = squared
            inverse = inverse_ref[...]
            inverse_ref[...] = inverse + three_products(inverse, squared)
        return left * left, count + 1

    lax.while_loop(more, double, (ratio * ratio, jnp.int32(0)))

    def newton(_, carry):
        gaps = [identity - full_product(s, ref[...]) for s, ref in zip(systems, inverse_refs)]
        for gap, inverse_ref in zip(gaps, inverse_refs):
            inverse = inverse_ref[...]
            inverse_ref[...] = inverse + full_product(inverse, gap)
        return carry

    lax.fori_loop(0, jnp.where(largest < 8.0, 1, 3), newton, 0)
    inverses = [ref[...] for ref in inverse_refs]
    uppers = [full_product(x, e) for x, e in zip(inverses, couplings)]
    lowers = [full_product(e, y, ((0,), (0,))) for e, y in zip(couplings, uppers)]
    return [
        (2.0 * x - identity, 2.0 * y, -2.0 * y.T, identity - 2.0 * z)
        for x, y, z in zip(inverses, uppers, lowers)
    ]


def store_halves(high_ref, low_ref, at_row, at_col, value):
    rows, cols = value.shape
    high, low = halves(value)
    high_ref[at_row : at_row + rows, at_col : at_col + cols] = high
    low_ref[at_row : at_row + rows, at_col : at_col + cols] = low


def step_one_matrices(gathered, norms, swap, rows_all):
    cols = gathered.shape[2]

    def kernel(swap_ref, cross_ref, norms_ref, high_ref, low_ref, power_ref, inverse_ref):
        cross = cross_ref[...].reshape(cols, cols)
        edge = (cross, norms_ref[...], 1.0)
        blocks = cayley([edge], rows_all, [power_ref], [inverse_ref])[0]
        turned = swap_ref[0] != 0
        for line in range(2):
            near, far = blocks[2 * line], blocks[2 * line + 1]
            store_halves(high_ref, low_ref, line * cols, 0, jnp.where(turned, far, near))
            store_halves(high_ref, low_ref, line * cols, cols, jnp.where(turned, near, far))

    out = jax.ShapeDtypeStruct((2 * cols, 2 * cols), BF16)
    vmem = pl.BlockSpec(memory_space=pltpu.VMEM)
    return pl.pallas_call(
        kernel,
        in_specs=[pl.BlockSpec(memory_space=pltpu.SMEM), vmem, vmem],
        out_shape=(out, out),
        scratch_shapes=[pltpu.VMEM((cols, cols), F32)] * 2,
        name="cayley_one",
    )(swap, gathered, norms)


def step_two_matrices(gathered, norms, other_norms, marks, rows_all):
    _, both, cols = gathered.shape
    per = both // 2

    def kernel(marks_ref, cross_ref, norms_ref, other_ref, *refs):
        outs, power_refs, inverse_refs = refs[:4], refs[4:6], refs[6:]
        edges = []
        for edge in range(2):
            cross = cross_ref[:, edge * per : (edge + 1) * per, :].reshape(cols, cols)
            sign = jnp.where(marks_ref[2 * edge] != 0, 1.0, -1.0).astype(F32)
            edges.append((cross, (norms_ref, other_ref)[edge][...], sign))
        for edge, blocks in enumerate(cayley(edges, rows_all, power_refs, inverse_refs)):
            moved_role = marks_ref[2 * edge + 1] != 0
            for line in range(2):
                value = jnp.where(moved_role, blocks[2 * line], blocks[2 * line + 1])
                store_halves(outs[2 * edge], outs[2 * edge + 1], line * cols, 0, value)

    out = jax.ShapeDtypeStruct((2 * cols, cols), BF16)
    vmem = pl.BlockSpec(memory_space=pltpu.VMEM)
    return pl.pallas_call(
        kernel,
        in_specs=[pl.BlockSpec(memory_space=pltpu.SMEM), vmem, vmem, vmem],
        out_shape=(out,) * 4,
        scratch_shapes=[pltpu.VMEM((cols, cols), F32)] * 4,
        name="cayley_two",
    )(marks, gathered, norms, other_norms)


def rotate(both, high, low, part, start, rows, block=512):
    width = both.shape[1]
    cols = width // 2

    def kernel(x_ref, high_ref, low_ref, out_ref):
        x_high, x_low = halves(x_ref[...])
        out_ref[...] = product(x_high, high_ref[...]) + (
            product(x_high, low_ref[...]) + product(x_low, high_ref[...])
        )

    at = start // block
    fixed = pl.BlockSpec((width, cols), lambda i: (0, part))
    return pl.pallas_call(
        kernel,
        grid=(rows // block,),
        in_specs=[pl.BlockSpec((block, width), lambda i: (i + at, 0)), fixed, fixed],
        out_specs=pl.BlockSpec((block, cols), lambda i: (i, 0)),
        out_shape=jax.ShapeDtypeStruct((rows, cols), F32),
        name="rotate",
    )(both, high, low)


def combine(at, lefts, rights, high, low, start, rows, before=None, block=512):
    cols = lefts[0].shape[1]
    steps = [x.shape[0] // block for x in lefts]
    begins = [sum(steps[:k]) for k in range(len(steps))]
    pieces, first = len(steps), start // block

    def kernel(at_ref, *refs):
        high_ref, low_ref, out_ref = refs[2 * pieces], refs[2 * pieces + 1], refs[-1]
        step = pl.program_id(0)
        for k in range(pieces):

            @pl.when((step >= begins[k]) & (step < begins[k] + steps[k]))
            def _(k=k):
                total = None
                for line, ref in enumerate((refs[k], refs[pieces + k])):
                    x_high, x_low = halves(ref[...])
                    m_high = high_ref[line * cols : (line + 1) * cols, :]
                    m_low = low_ref[line * cols : (line + 1) * cols, :]
                    part = product(x_high, m_high) + (
                        product(x_high, m_low) + product(x_low, m_high)
                    )
                    total = part if total is None else total + part
                out_ref[...] = total

    data = [
        pl.BlockSpec((block, cols), lambda i, at_ref, b=b, n=n: (jnp.clip(i - b, 0, n - 1), 0))
        for b, n in zip(begins, steps)
    ]
    fixed = pl.BlockSpec((2 * cols, cols), lambda i, at_ref: (0, 0))
    operands = [at, *lefts, *rights, high, low]
    in_specs = [*data, *data, fixed, fixed]
    aliases = {}
    if before is not None:
        operands.append(before)
        in_specs.append(pl.BlockSpec(memory_space=pl.ANY))
        aliases = {len(operands) - 1: 0}
    return pl.pallas_call(
        kernel,
        grid_spec=pltpu.PrefetchScalarGridSpec(
            num_scalar_prefetch=1,
            grid=(sum(steps),),
            in_specs=in_specs,
            out_specs=pl.BlockSpec((block, cols), lambda i, at_ref: (i + first, at_ref[0])),
        ),
        out_shape=jax.ShapeDtypeStruct((rows, 2 * cols), F32),
        input_output_aliases=aliases,
        name="combine",
    )(*operands)


def exchanged(blocks, groups=None):
    return lax.all_to_all(blocks, "rows", 0, 0, axis_index_groups=groups, tiled=True)


def held(value, *until):
    return lax.optimization_barrier((value, *until))[0]


def shards(matrix):
    cols = matrix.shape[1] // 2
    rows = matrix.shape[0]
    peers = lax.axis_size("rows")
    rows_all = rows * peers
    per = cols // peers
    position = lax.axis_index("pairs")
    size = lax.axis_size("pairs")
    ring = [*range(0, size, 2), *range(size - 1, 0, -2)]
    clockwise = [(ring[i], ring[(i + 1) % size]) for i in range(size)]
    back = [(b, a) for a, b in clockwise]
    even = position % 2 == 0
    pieces = [(0, rows // 2), (rows // 2, rows // 4), (3 * rows // 4, rows // 4)]

    slabs = exchanged(gram(matrix, 0, matrix, 1, rows, peers, cols, block=rows // 2))
    spread, norms = slab_sum(slabs, cols, True)
    gathered = exchanged(spread)
    swap = jnp.where(even & (position > 0), 0, 1).astype(jnp.int32)[None]
    high, low = step_one_matrices(gathered, norms, swap, float(rows_all))
    onward, arrived = [], []
    for k, piece in enumerate(pieces):
        onward.append(rotate(matrix, high, low, 0, *piece))
        arrived.append(lax.ppermute(onward[k], "pairs", clockwise))
    kept = [rotate(matrix, high, low, 1, *piece) for piece in pieces]

    line = peers // 2
    halves_of_rows = [[*range(line)], [*range(line, peers)]]
    across = [(i, (i + line) % peers) for i in range(peers)]
    per = cols // line
    begun = ()
    for k in range(2):
        begun = gram_parts(arrived[k : k + 1], kept[k : k + 1], cols, begun)
    slabs = gram(arrived[2], 0, kept[2], 0, pieces[2][1], line, cols, begun)
    returned = [None] * 3
    returned[1] = lax.ppermute(held(kept[1], slabs), "pairs", back)
    slabs = exchanged(slabs, halves_of_rows)
    mine, _ = slab_sum(slabs, cols, False)
    other = lax.ppermute(mine, "pairs", back)
    partner = lax.ppermute(jnp.concatenate([mine, other], axis=0), "rows", across)
    for at in (0, 2):
        returned[at] = lax.ppermute(held(kept[at], partner), "pairs", back)
    pair, norms, other_norms = paired(mine, other, partner, line, per)
    gathered = exchanged(pair, halves_of_rows)
    marks = jnp.stack(
        [
            (even & (position > 0)) | (position == size - 1),
            position != 0,
            even,
            position == 1,
        ]
    ).astype(jnp.int32)
    matrices = step_two_matrices(gathered, norms, other_norms, marks, float(rows_all))
    in_first = jnp.where(even, 0, 1).astype(jnp.int32)[None]
    done = combine(in_first, arrived, kept, *matrices[:2], 0, rows)
    for k in (slice(0, 2), slice(2, 3)):
        done = combine(
            1 - in_first, onward[k], returned[k], *matrices[2:], pieces[k.start][0], rows, done
        )
    return done


def solution(mesh):
    return jax.shard_map(
        shards,
        mesh=mesh,
        in_specs=(P("rows", "pairs"),),
        out_specs=P("rows", "pairs"),
        check_vma=False,
    )
```

```python
import jax
import jax.numpy as jnp
from jax import lax
from jax.experimental import pallas as pl
from jax.experimental.pallas import tpu as pltpu
from jax.sharding import PartitionSpec as P


F32, BF16 = jnp.float32, jnp.bfloat16
TAIL = 8
LANES = 128
BLOCK = 512


def halves(x):
    high = x.astype(BF16)
    return high, (x - high.astype(F32)).astype(BF16)


def product(a, b, dims=((1,), (0,))):
    return lax.dot_general(a, b, (dims, ((), ())), preferred_element_type=F32)


def three_products(a, b, dims=((1,), (0,))):
    (a_high, a_low), (b_high, b_low) = halves(a), halves(b)
    return product(a_high, b_high, dims) + (product(a_high, b_low, dims) + product(a_low, b_high, dims))


def full_product(a, b, dims=((1,), (0,))):
    return lax.dot_general(
        a, b, (dims, ((), ())), precision=lax.Precision.HIGHEST, preferred_element_type=F32
    )


def gram_parts(lefts, rights, cols, before=()):
    pieces = len(lefts)

    def kernel(*refs):
        ins, (acc_ref, norms_ref) = refs[:-2], refs[-2:]
        acc = norms = None
        for a_ref, b_ref in zip(ins[:pieces], ins[pieces : 2 * pieces]):
            a, b = a_ref[...], b_ref[...]
            part = three_products(a, b, ((0,), (0,)))
            squares = jnp.concatenate([a * a, b * b], axis=1)
            squares = jnp.sum(squares.reshape(a.shape[0] // 8, 8, 2 * cols), axis=0)
            acc = part if acc is None else acc + part
            norms = squares if norms is None else norms + squares
        if before:
            acc, norms = acc + ins[-2][...], norms + ins[-1][...]
        acc_ref[...] = acc
        norms_ref[...] = norms

    return pl.pallas_call(
        kernel,
        out_shape=(
            jax.ShapeDtypeStruct((cols, cols), F32),
            jax.ShapeDtypeStruct((8, 2 * cols), F32),
        ),
        name="gram_parts",
    )(*lefts, *rights, *before)


def store_slabs(out_ref, acc_ref, norms, peers, cols):
    per, wide = cols // peers, cols // LANES
    total = jnp.sum(norms, axis=0, keepdims=True)
    lines = [total[:, LANES * q : LANES * (q + 1)] for q in range(2 * wide)]
    tail = jnp.concatenate([*lines, jnp.zeros((TAIL - 2 * wide, LANES), F32)], axis=0)
    for peer in range(peers):
        rows = acc_ref[peer * per : (peer + 1) * per, :]
        for q in range(wide):
            out_ref[peer, q * per : (q + 1) * per, :] = rows[:, LANES * q : LANES * (q + 1)]
        out_ref[peer, wide * per :, :] = tail


def gram(left, left_at, right, right_at, rows, peers, cols, before=(), block=512):
    per, wide = cols // peers, cols // LANES

    def kernel(left_ref, right_ref, *refs):
        out_ref, acc_ref, norms_ref = refs[-3:]
        step = pl.program_id(0)

        @pl.when(step == 0)
        def _():
            if before:
                acc_ref[...] = refs[0][...]
                norms_ref[...] = refs[1][...]
            else:
                acc_ref[...] = jnp.zeros_like(acc_ref)
                norms_ref[...] = jnp.zeros_like(norms_ref)

        a, b = left_ref[...], right_ref[...]
        acc_ref[...] += three_products(a, b, ((0,), (0,)))
        norms_ref[:, :cols] += jnp.sum((a * a).reshape(block // 8, 8, cols), axis=0)
        norms_ref[:, cols:] += jnp.sum((b * b).reshape(block // 8, 8, cols), axis=0)

        @pl.when(step == pl.num_programs(0) - 1)
        def _():
            store_slabs(out_ref, acc_ref, norms_ref[...], peers, cols)

    shape = (peers, wide * per + TAIL, LANES)
    return pl.pallas_call(
        kernel,
        grid=(rows // block,),
        in_specs=[
            pl.BlockSpec((block, cols), lambda i: (i, left_at)),
            pl.BlockSpec((block, cols), lambda i: (i, right_at)),
            *[pl.BlockSpec(x.shape, lambda i: (0, 0)) for x in before],
        ],
        out_specs=pl.BlockSpec(shape, lambda i: (0, 0, 0)),
        out_shape=jax.ShapeDtypeStruct(shape, F32),
        scratch_shapes=[pltpu.VMEM((cols, cols), F32), pltpu.VMEM((8, 2 * cols), F32)],
        name="gram",
    )(left, right, *before)


def slab_sum(slabs, cols, spread):
    peers = slabs.shape[0]
    per, wide = cols // peers, cols // LANES

    def kernel(in_ref, out_ref, norms_ref):
        total = in_ref[0]
        for peer in range(1, peers):
            total = total + in_ref[peer]
        rows = jnp.concatenate([total[q * per : (q + 1) * per] for q in range(wide)], axis=1)
        if spread:
            for peer in range(peers):
                out_ref[peer] = rows
        else:
            out_ref[:per] = rows
        tail = total[wide * per :]
        norms = []
        for side in range(2):
            lines = [tail[side * wide + q : side * wide + q + 1] for q in range(wide)]
            norms.append(jnp.concatenate(lines, axis=1))
        norms = jnp.concatenate([*norms, jnp.zeros((TAIL - 2, cols), F32)], axis=0)
        norms_ref[...] = norms
        if not spread:
            out_ref[per:] = norms

    shape = (peers, per, cols) if spread else (per + TAIL, cols)
    return pl.pallas_call(
        kernel,
        out_shape=(jax.ShapeDtypeStruct(shape, F32), jax.ShapeDtypeStruct((TAIL, cols), F32)),
        name="slab_sum",
    )(slabs)


def paired(mine, partner, other, far, peers, per):
    cols = mine.shape[1]

    def kernel(mine_ref, partner_ref, other_ref, far_ref, out_ref, norms_ref, other_norms_ref):
        own = mine_ref[...] + partner_ref[...]
        theirs = other_ref[...] + far_ref[...]
        for peer in range(peers):
            out_ref[peer, :per] = own[:per]
            out_ref[peer, per:] = theirs[:per]
        norms_ref[...] = own[per:]
        other_norms_ref[...] = theirs[per:]

    norms = jax.ShapeDtypeStruct((TAIL, cols), F32)
    return pl.pallas_call(
        kernel,
        out_shape=(jax.ShapeDtypeStruct((peers, 2 * per, cols), F32), norms, norms),
        name="paired",
    )(mine, partner, other, far)


def cayley(edges, rows_all, power_refs, inverse_refs):
    cols = edges[0][0].shape[0]
    row_at = lax.broadcasted_iota(jnp.int32, (cols, cols), 0)
    col_at = lax.broadcasted_iota(jnp.int32, (cols, cols), 1)
    diagonal = row_at == col_at
    identity = jnp.where(diagonal, 1.0, 0.0).astype(F32)
    couplings, systems, bounds = [], [], []
    for cross, norms, sign in edges:
        scale_left = lax.rsqrt(norms[0:1] / rows_all + 1e-06)
        scale_right = lax.rsqrt(norms[1:2] / rows_all + 1e-06)
        spread = jnp.where(diagonal, jnp.broadcast_to(scale_left, (cols, cols)), 0.0)
        scale_left = jnp.sum(spread, axis=1, keepdims=True)
        coupling = (0.5 * sign) * cross * scale_left * scale_right / rows_all
        couplings.append(coupling)
        systems.append(identity + full_product(coupling, coupling, ((1,), (1,))))
    for system, power_ref, inverse_ref in zip(systems, power_refs, inverse_refs):
        bound = jnp.max(jnp.sum(jnp.abs(system), axis=0, keepdims=True))
        factor = 2.0 / (1.0 + bound)
        power = identity - factor * system
        inverse_ref[...] = factor * (identity + power)
        power_ref[...] = power
        bounds.append(bound)
    largest = bounds[0] if len(bounds) == 1 else jnp.maximum(*bounds)
    ratio = (largest - 1.0) / (largest + 1.0)

    def more(carry):
        left, count = carry
        return (left > 1e-3) & (count < 40)

    def double(carry):
        left, count = carry
        squares = []
        for power_ref in power_refs:
            before = power_ref[...]
            squares.append(three_products(before, before))
        for squared, power_ref, inverse_ref in zip(squares, power_refs, inverse_refs):
            power_ref[...] = squared
            inverse = inverse_ref[...]
            inverse_ref[...] = inverse + three_products(inverse, squared)
        return left * left, count + 1

    lax.while_loop(more, double, (ratio * ratio, jnp.int32(0)))

    def newton(_, carry):
        gaps = [identity - full_product(s, ref[...]) for s, ref in zip(systems, inverse_refs)]
        for gap, inverse_ref in zip(gaps, inverse_refs):
            inverse = inverse_ref[...]
            inverse_ref[...] = inverse + full_product(inverse, gap)
        return carry

    lax.fori_loop(0, jnp.where(largest < 8.0, 1, 3), newton, 0)
    inverses = [ref[...] for ref in inverse_refs]
    uppers = [full_product(x, e) for x, e in zip(inverses, couplings)]
    lowers = [full_product(e, y, ((0,), (0,))) for e, y in zip(couplings, uppers)]
    return [
        (2.0 * x - identity, 2.0 * y, -2.0 * y.T, identity - 2.0 * z)
        for x, y, z in zip(inverses, uppers, lowers)
    ]


def store_halves(high_ref, low_ref, at_row, at_col, value):
    rows, cols = value.shape
    high, low = halves(value)
    high_ref[at_row : at_row + rows, at_col : at_col + cols] = high
    low_ref[at_row : at_row + rows, at_col : at_col + cols] = low


def step_one_matrices(gathered, norms, swap, matrix, rows, rows_all):
    cols = gathered.shape[2]

    def kernel(swap_ref, cross_ref, norms_ref, x_in, high_ref, low_ref, first_ref, *refs):
        power_ref, inverse_ref, x_ref, sem = refs
        copy = pltpu.make_async_copy(x_in.at[pl.ds(0, rows), :], x_ref, sem)
        copy.start()
        cross = cross_ref[...].reshape(cols, cols)
        edge = (cross, norms_ref[...], 1.0)
        blocks = cayley([edge], rows_all, [power_ref], [inverse_ref])[0]
        turned = swap_ref[0] != 0
        for line in range(2):
            near, far = blocks[2 * line], blocks[2 * line + 1]
            store_halves(high_ref, low_ref, line * cols, 0, jnp.where(turned, far, near))
            store_halves(high_ref, low_ref, line * cols, cols, jnp.where(turned, near, far))
        copy.wait()
        x_high, x_low = halves(x_ref[...])
        m_high, m_low = high_ref[:, :cols], low_ref[:, :cols]
        first_ref[...] = product(x_high, m_high) + (
            product(x_high, m_low) + product(x_low, m_high)
        )

    out = jax.ShapeDtypeStruct((2 * cols, 2 * cols), BF16)
    vmem = pl.BlockSpec(memory_space=pltpu.VMEM)
    return pl.pallas_call(
        kernel,
        in_specs=[
            pl.BlockSpec(memory_space=pltpu.SMEM),
            vmem,
            vmem,
            pl.BlockSpec(memory_space=pl.ANY),
        ],
        out_shape=(out, out, jax.ShapeDtypeStruct((rows, cols), F32)),
        scratch_shapes=[
            pltpu.VMEM((cols, cols), F32),
            pltpu.VMEM((cols, cols), F32),
            pltpu.VMEM((rows, 2 * cols), F32),
            pltpu.SemaphoreType.DMA,
        ],
        name="cayley_one",
    )(swap, gathered, norms, matrix)


def step_two(gathered, norms, other_norms, marks, received, sent, rows, rows_all, block):
    _, both, cols = gathered.shape
    per = both // 2
    pieces = [(0, *p) for p in received] + [(1, *p) for p in sent]
    places = [
        (edge, k, row, n * block)
        for k, (edge, row, left, _) in enumerate(pieces)
        for n in range(left.shape[0] // block)
    ]
    blocks = len(places)

    def kernel(marks_ref, cross_ref, norms_ref, other_ref, *refs):
        ins = refs[: 2 * len(pieces)]
        out_ref, high_ref, low_ref = refs[2 * len(pieces) : 2 * len(pieces) + 3]
        power_refs, inverse_refs = refs[-10:-8], refs[-8:-6]
        data_ref, turned_ref, own_high, own_low, in_sems, out_sems = refs[-6:]
        loads = []
        for i, (_, k, _, begin) in enumerate(places):
            for side in range(2):
                load = pltpu.make_async_copy(
                    ins[2 * k + side].at[pl.ds(begin, block), :],
                    data_ref.at[i, :, pl.ds(side * cols, cols)],
                    in_sems.at[2 * i + side],
                )
                load.start()
                loads.append(load)
        edges = []
        for edge in range(2):
            cross = cross_ref[:, edge * per : (edge + 1) * per, :].reshape(cols, cols)
            sign = jnp.where(marks_ref[2 * edge] != 0, 1.0, -1.0).astype(F32)
            edges.append((cross, (norms_ref, other_ref)[edge][...], sign))
        matrices = ((own_high, own_low), (high_ref, low_ref))
        for edge, turns in enumerate(cayley(edges, rows_all, power_refs, inverse_refs)):
            moved_role = marks_ref[2 * edge + 1] != 0
            for half in range(2):
                value = jnp.where(moved_role, turns[2 * half], turns[2 * half + 1])
                store_halves(*matrices[edge], half * cols, 0, value)
        columns = [
            pl.multiple_of(marks_ref[4] * cols, cols),
            pl.multiple_of((1 - marks_ref[4]) * cols, cols),
        ]
        stores = []
        for i, (edge, _, row, begin) in enumerate(places):
            loads[2 * i].wait()
            loads[2 * i + 1].wait()
            x_high, x_low = halves(data_ref[i])
            m_high, m_low = matrices[edge]
            turned_ref[i] = product(x_high, m_high[...]) + (
                product(x_high, m_low[...]) + product(x_low, m_high[...])
            )
            store = pltpu.make_async_copy(
                turned_ref.at[i],
                out_ref.at[pl.ds(row + begin, block), pl.ds(columns[edge], cols)],
                out_sems.at[i],
            )
            store.start()
            stores.append(store)
        for store in stores:
            store.wait()

    out = jax.ShapeDtypeStruct((2 * cols, cols), BF16)
    vmem = pl.BlockSpec(memory_space=pltpu.VMEM)
    anywhere = pl.BlockSpec(memory_space=pl.ANY)
    return pl.pallas_call(
        kernel,
        in_specs=[
            pl.BlockSpec(memory_space=pltpu.SMEM),
            vmem,
            vmem,
            vmem,
            *[anywhere] * (2 * len(pieces)),
        ],
        out_specs=(anywhere, vmem, vmem),
        out_shape=(jax.ShapeDtypeStruct((rows, 2 * cols), F32), out, out),
        scratch_shapes=[
            *[pltpu.VMEM((cols, cols), F32)] * 4,
            pltpu.VMEM((blocks, block, 2 * cols), F32),
            pltpu.VMEM((blocks, block, cols), F32),
            pltpu.VMEM((2 * cols, cols), BF16),
            pltpu.VMEM((2 * cols, cols), BF16),
            pltpu.SemaphoreType.DMA((2 * blocks,)),
            pltpu.SemaphoreType.DMA((blocks,)),
        ],
        name="step_two",
    )(marks, gathered, norms, other_norms, *[x for p in pieces for x in p[2:]])


def rotate(both, high, low, part, start, rows, block=512):
    width = both.shape[1]
    cols = width // 2

    def kernel(x_ref, high_ref, low_ref, out_ref):
        x_high, x_low = halves(x_ref[...])
        out_ref[...] = product(x_high, high_ref[...]) + (
            product(x_high, low_ref[...]) + product(x_low, high_ref[...])
        )

    at = start // block
    fixed = pl.BlockSpec((width, cols), lambda i: (0, part))
    return pl.pallas_call(
        kernel,
        grid=(rows // block,),
        in_specs=[pl.BlockSpec((block, width), lambda i: (i + at, 0)), fixed, fixed],
        out_specs=pl.BlockSpec((block, cols), lambda i: (i, 0)),
        out_shape=jax.ShapeDtypeStruct((rows, cols), F32),
        name="rotate",
    )(both, high, low)


def combine(at, lefts, rights, high, low, start, rows, before=None, block=512):
    cols = lefts[0].shape[1]
    steps = [x.shape[0] // block for x in lefts]
    begins = [sum(steps[:k]) for k in range(len(steps))]
    pieces, first = len(steps), start // block

    def kernel(at_ref, *refs):
        high_ref, low_ref, out_ref = refs[2 * pieces], refs[2 * pieces + 1], refs[-1]
        step = pl.program_id(0)
        for k in range(pieces):

            @pl.when((step >= begins[k]) & (step < begins[k] + steps[k]))
            def _(k=k):
                total = None
                for line, ref in enumerate((refs[k], refs[pieces + k])):
                    x_high, x_low = halves(ref[...])
                    m_high = high_ref[line * cols : (line + 1) * cols, :]
                    m_low = low_ref[line * cols : (line + 1) * cols, :]
                    part = product(x_high, m_high) + (
                        product(x_high, m_low) + product(x_low, m_high)
                    )
                    total = part if total is None else total + part
                out_ref[...] = total

    data = [
        pl.BlockSpec((block, cols), lambda i, at_ref, b=b, n=n: (jnp.clip(i - b, 0, n - 1), 0))
        for b, n in zip(begins, steps)
    ]
    fixed = pl.BlockSpec((2 * cols, cols), lambda i, at_ref: (0, 0))
    operands = [at, *lefts, *rights, high, low]
    in_specs = [*data, *data, fixed, fixed]
    aliases = {}
    if before is not None:
        operands.append(before)
        in_specs.append(pl.BlockSpec(memory_space=pl.ANY))
        aliases = {len(operands) - 1: 0}
    return pl.pallas_call(
        kernel,
        grid_spec=pltpu.PrefetchScalarGridSpec(
            num_scalar_prefetch=1,
            grid=(sum(steps),),
            in_specs=in_specs,
            out_specs=pl.BlockSpec((block, cols), lambda i, at_ref: (i + first, at_ref[0])),
        ),
        out_shape=jax.ShapeDtypeStruct((rows, 2 * cols), F32),
        input_output_aliases=aliases,
        name="combine",
    )(*operands)


def exchanged(blocks, groups=None):
    return lax.all_to_all(blocks, "rows", 0, 0, axis_index_groups=groups, tiled=True)


def held(value, *until):
    return lax.optimization_barrier((value, *until))[0]


def shards(matrix):
    cols = matrix.shape[1] // 2
    rows = matrix.shape[0]
    peers = lax.axis_size("rows")
    rows_all = rows * peers
    per = cols // peers
    position = lax.axis_index("pairs")
    size = lax.axis_size("pairs")
    ring = [*range(0, size, 2), *range(size - 1, 0, -2)]
    clockwise = [(ring[i], ring[(i + 1) % size]) for i in range(size)]
    back = [(b, a) for a, b in clockwise]
    even = position % 2 == 0
    pieces = [(0, rows // 4), (rows // 4, rows // 2), (3 * rows // 4, rows // 4)]

    slabs = exchanged(gram(matrix, 0, matrix, 1, rows, peers, cols, block=rows // 2))
    spread, norms = slab_sum(slabs, cols, True)
    gathered = exchanged(spread)
    swap = jnp.where(even & (position > 0), 0, 1).astype(jnp.int32)[None]
    high, low, turned = step_one_matrices(
        gathered, norms, swap, matrix, pieces[0][1], float(rows_all)
    )
    onward, arrived = [turned], []
    for k, piece in enumerate(pieces):
        if k:
            onward.append(rotate(matrix, high, low, 0, *piece))
        arrived.append(lax.ppermute(onward[k], "pairs", clockwise))
    kept = [rotate(matrix, high, low, 1, *piece) for piece in pieces]

    line = peers // 2
    halves_of_rows = [[*range(line)], [*range(line, peers)]]
    across = [(i, (i + line) % peers) for i in range(peers)]
    both_ways = [(r * size + b, q * size + a) for r, q in across for b, a in back]
    per = cols // line
    begun = ()
    for k in range(2):
        begun = gram_parts(arrived[k : k + 1], kept[k : k + 1], cols, begun)
    slabs = gram(arrived[2], 0, kept[2], 0, pieces[2][1], line, cols, begun)
    returned = [None] * 3
    returned[0] = lax.ppermute(held(kept[0], slabs), "pairs", back)
    slabs = exchanged(slabs, halves_of_rows)
    mine, _ = slab_sum(slabs, cols, False)
    other = lax.ppermute(mine, "pairs", back)
    partner = lax.ppermute(mine, "rows", across)
    far = lax.ppermute(mine, ("rows", "pairs"), both_ways)
    for at in (2, 1):
        returned[at] = lax.ppermute(held(kept[at], far, partner, other), "pairs", back)
    pair, norms, other_norms = paired(mine, partner, other, far, line, per)
    gathered = exchanged(pair, halves_of_rows)
    in_second = ~even
    marks = jnp.stack(
        [
            (even & (position > 0)) | (position == size - 1),
            position != 0,
            even,
            position == 1,
            in_second,
        ]
    ).astype(jnp.int32)
    begins = [begin for begin, _ in pieces]
    received = list(zip(begins, arrived, kept))
    sent = [(begins[k], onward[k], returned[k]) for k in (0, 2)]
    done, high, low = step_two(
        gathered, norms, other_norms, marks, received, sent, rows, float(rows_all), BLOCK
    )
    in_first = even.astype(jnp.int32)[None]
    return combine(
        in_first, onward[1:2], returned[1:2], high, low, begins[1], rows, done
    )


def solution(mesh):
    return jax.shard_map(
        shards,
        mesh=mesh,
        in_specs=(P("rows", "pairs"),),
        out_specs=P("rows", "pairs"),
        check_vma=False,
    )
```

```python
import jax
import jax.numpy as jnp
from jax import lax
from jax.experimental import pallas as pl
from jax.experimental.pallas import tpu as pltpu
from jax.sharding import PartitionSpec as P


F32, BF16 = jnp.float32, jnp.bfloat16
TAIL = 8
LANES = 128
BLOCK = 512


def halves(x):
    high = x.astype(BF16)
    return high, (x - high.astype(F32)).astype(BF16)


def product(a, b, dims=((1,), (0,))):
    return lax.dot_general(a, b, (dims, ((), ())), preferred_element_type=F32)


def three_products(a, b, dims=((1,), (0,))):
    (a_high, a_low), (b_high, b_low) = halves(a), halves(b)
    return product(a_high, b_high, dims) + (product(a_high, b_low, dims) + product(a_low, b_high, dims))


def full_product(a, b, dims=((1,), (0,))):
    return lax.dot_general(
        a, b, (dims, ((), ())), precision=lax.Precision.HIGHEST, preferred_element_type=F32
    )


def gram_parts(lefts, rights, cols, before=()):
    pieces = len(lefts)

    def kernel(*refs):
        ins, (acc_ref, norms_ref) = refs[:-2], refs[-2:]
        acc = norms = None
        for a_ref, b_ref in zip(ins[:pieces], ins[pieces : 2 * pieces]):
            a, b = a_ref[...], b_ref[...]
            part = three_products(a, b, ((0,), (0,)))
            squares = jnp.concatenate([a * a, b * b], axis=1)
            squares = jnp.sum(squares.reshape(a.shape[0] // 8, 8, 2 * cols), axis=0)
            acc = part if acc is None else acc + part
            norms = squares if norms is None else norms + squares
        if before:
            acc, norms = acc + ins[-2][...], norms + ins[-1][...]
        acc_ref[...] = acc
        norms_ref[...] = norms

    return pl.pallas_call(
        kernel,
        out_shape=(
            jax.ShapeDtypeStruct((cols, cols), F32),
            jax.ShapeDtypeStruct((8, 2 * cols), F32),
        ),
        name="gram_parts",
    )(*lefts, *rights, *before)


def store_slabs(out_ref, acc_ref, norms, peers, cols):
    per, wide = cols // peers, cols // LANES
    total = jnp.sum(norms, axis=0, keepdims=True)
    lines = [total[:, LANES * q : LANES * (q + 1)] for q in range(2 * wide)]
    tail = jnp.concatenate([*lines, jnp.zeros((TAIL - 2 * wide, LANES), F32)], axis=0)
    for peer in range(peers):
        rows = acc_ref[peer * per : (peer + 1) * per, :]
        for q in range(wide):
            out_ref[peer, q * per : (q + 1) * per, :] = rows[:, LANES * q : LANES * (q + 1)]
        out_ref[peer, wide * per :, :] = tail


def gram(left, left_at, right, right_at, rows, peers, cols, before=(), block=512):
    per, wide = cols // peers, cols // LANES

    def kernel(left_ref, right_ref, *refs):
        out_ref, acc_ref, norms_ref = refs[-3:]
        step = pl.program_id(0)

        @pl.when(step == 0)
        def _():
            if before:
                acc_ref[...] = refs[0][...]
                norms_ref[...] = refs[1][...]
            else:
                acc_ref[...] = jnp.zeros_like(acc_ref)
                norms_ref[...] = jnp.zeros_like(norms_ref)

        a, b = left_ref[...], right_ref[...]
        acc_ref[...] += three_products(a, b, ((0,), (0,)))
        norms_ref[:, :cols] += jnp.sum((a * a).reshape(block // 8, 8, cols), axis=0)
        norms_ref[:, cols:] += jnp.sum((b * b).reshape(block // 8, 8, cols), axis=0)

        @pl.when(step == pl.num_programs(0) - 1)
        def _():
            store_slabs(out_ref, acc_ref, norms_ref[...], peers, cols)

    shape = (peers, wide * per + TAIL, LANES)
    return pl.pallas_call(
        kernel,
        grid=(rows // block,),
        in_specs=[
            pl.BlockSpec((block, cols), lambda i: (i, left_at)),
            pl.BlockSpec((block, cols), lambda i: (i, right_at)),
            *[pl.BlockSpec(x.shape, lambda i: (0, 0)) for x in before],
        ],
        out_specs=pl.BlockSpec(shape, lambda i: (0, 0, 0)),
        out_shape=jax.ShapeDtypeStruct(shape, F32),
        scratch_shapes=[pltpu.VMEM((cols, cols), F32), pltpu.VMEM((8, 2 * cols), F32)],
        name="gram",
    )(left, right, *before)


def slab_sum(slabs, cols, spread):
    peers = slabs.shape[0]
    per, wide = cols // peers, cols // LANES

    def kernel(in_ref, out_ref, norms_ref):
        total = in_ref[0]
        for peer in range(1, peers):
            total = total + in_ref[peer]
        rows = jnp.concatenate([total[q * per : (q + 1) * per] for q in range(wide)], axis=1)
        if spread:
            for peer in range(peers):
                out_ref[peer] = rows
        else:
            out_ref[:per] = rows
        tail = total[wide * per :]
        norms = []
        for side in range(2):
            lines = [tail[side * wide + q : side * wide + q + 1] for q in range(wide)]
            norms.append(jnp.concatenate(lines, axis=1))
        norms = jnp.concatenate([*norms, jnp.zeros((TAIL - 2, cols), F32)], axis=0)
        norms_ref[...] = norms
        if not spread:
            out_ref[per:] = norms

    shape = (peers, per, cols) if spread else (per + TAIL, cols)
    return pl.pallas_call(
        kernel,
        out_shape=(jax.ShapeDtypeStruct(shape, F32), jax.ShapeDtypeStruct((TAIL, cols), F32)),
        name="slab_sum",
    )(slabs)


def paired(mine, partner, other, far, peers, per):
    cols = mine.shape[1]

    def kernel(mine_ref, partner_ref, other_ref, far_ref, out_ref, norms_ref, other_norms_ref):
        own = mine_ref[...] + partner_ref[...]
        theirs = other_ref[...] + far_ref[...]
        for peer in range(peers):
            out_ref[peer, :per] = own[:per]
            out_ref[peer, per:] = theirs[:per]
        norms_ref[...] = own[per:]
        other_norms_ref[...] = theirs[per:]

    norms = jax.ShapeDtypeStruct((TAIL, cols), F32)
    return pl.pallas_call(
        kernel,
        out_shape=(jax.ShapeDtypeStruct((peers, 2 * per, cols), F32), norms, norms),
        name="paired",
    )(mine, partner, other, far)


def cayley(edges, rows_all, power_refs, inverse_refs):
    cols = edges[0][0].shape[0]
    row_at = lax.broadcasted_iota(jnp.int32, (cols, cols), 0)
    col_at = lax.broadcasted_iota(jnp.int32, (cols, cols), 1)
    diagonal = row_at == col_at
    identity = jnp.where(diagonal, 1.0, 0.0).astype(F32)
    couplings, systems, bounds = [], [], []
    for cross, norms, sign in edges:
        scale_left = lax.rsqrt(norms[0:1] / rows_all + 1e-06)
        scale_right = lax.rsqrt(norms[1:2] / rows_all + 1e-06)
        spread = jnp.where(diagonal, jnp.broadcast_to(scale_left, (cols, cols)), 0.0)
        scale_left = jnp.sum(spread, axis=1, keepdims=True)
        coupling = (0.5 * sign) * cross * scale_left * scale_right / rows_all
        couplings.append(coupling)
        systems.append(identity + full_product(coupling, coupling, ((1,), (1,))))
    for system, power_ref, inverse_ref in zip(systems, power_refs, inverse_refs):
        bound = jnp.max(jnp.sum(jnp.abs(system), axis=0, keepdims=True))
        factor = 2.0 / (1.0 + bound)
        power = identity - factor * system
        inverse_ref[...] = factor * (identity + power)
        power_ref[...] = power
        bounds.append(bound)
    largest = bounds[0] if len(bounds) == 1 else jnp.maximum(*bounds)
    ratio = (largest - 1.0) / (largest + 1.0)

    def more(carry):
        left, count = carry
        return (left > 1e-3) & (count < 40)

    def double(carry):
        left, count = carry
        squares = []
        for power_ref in power_refs:
            before = power_ref[...]
            squares.append(three_products(before, before))
        for squared, power_ref, inverse_ref in zip(squares, power_refs, inverse_refs):
            power_ref[...] = squared
            inverse = inverse_ref[...]
            inverse_ref[...] = inverse + three_products(inverse, squared)
        return left * left, count + 1

    lax.while_loop(more, double, (ratio * ratio, jnp.int32(0)))

    def newton(_, carry):
        gaps = [identity - full_product(s, ref[...]) for s, ref in zip(systems, inverse_refs)]
        for gap, inverse_ref in zip(gaps, inverse_refs):
            inverse = inverse_ref[...]
            inverse_ref[...] = inverse + three_products(inverse, gap)
        return carry

    lax.fori_loop(0, jnp.where(largest < 8.0, 1, 3), newton, 0)
    inverses = [ref[...] for ref in inverse_refs]
    uppers = [full_product(x, e) for x, e in zip(inverses, couplings)]
    lowers = [full_product(e, y, ((0,), (0,))) for e, y in zip(couplings, uppers)]
    return [
        (2.0 * x - identity, 2.0 * y, -2.0 * y.T, identity - 2.0 * z)
        for x, y, z in zip(inverses, uppers, lowers)
    ]


def store_halves(high_ref, low_ref, at_row, at_col, value):
    rows, cols = value.shape
    high, low = halves(value)
    high_ref[at_row : at_row + rows, at_col : at_col + cols] = high
    low_ref[at_row : at_row + rows, at_col : at_col + cols] = low


def step_one_matrices(gathered, norms, swap, matrix, rows, rows_all):
    cols = gathered.shape[2]

    def kernel(swap_ref, cross_ref, norms_ref, x_in, high_ref, low_ref, first_ref, *refs):
        power_ref, inverse_ref, x_ref, sem = refs
        copy = pltpu.make_async_copy(x_in.at[pl.ds(0, rows), :], x_ref, sem)
        copy.start()
        cross = cross_ref[...].reshape(cols, cols)
        edge = (cross, norms_ref[...], 1.0)
        blocks = cayley([edge], rows_all, [power_ref], [inverse_ref])[0]
        turned = swap_ref[0] != 0
        for line in range(2):
            near, far = blocks[2 * line], blocks[2 * line + 1]
            store_halves(high_ref, low_ref, line * cols, 0, jnp.where(turned, far, near))
            store_halves(high_ref, low_ref, line * cols, cols, jnp.where(turned, near, far))
        copy.wait()
        x_high, x_low = halves(x_ref[...])
        m_high, m_low = high_ref[:, :cols], low_ref[:, :cols]
        first_ref[...] = product(x_high, m_high) + (
            product(x_high, m_low) + product(x_low, m_high)
        )

    out = jax.ShapeDtypeStruct((2 * cols, 2 * cols), BF16)
    vmem = pl.BlockSpec(memory_space=pltpu.VMEM)
    return pl.pallas_call(
        kernel,
        in_specs=[
            pl.BlockSpec(memory_space=pltpu.SMEM),
            vmem,
            vmem,
            pl.BlockSpec(memory_space=pl.ANY),
        ],
        out_shape=(out, out, jax.ShapeDtypeStruct((rows, cols), F32)),
        scratch_shapes=[
            pltpu.VMEM((cols, cols), F32),
            pltpu.VMEM((cols, cols), F32),
            pltpu.VMEM((rows, 2 * cols), F32),
            pltpu.SemaphoreType.DMA,
        ],
        name="cayley_one",
    )(swap, gathered, norms, matrix)


def step_two(gathered, norms, other_norms, marks, received, sent, rows, rows_all, block):
    _, both, cols = gathered.shape
    per = both // 2
    pieces = [(0, *p) for p in received] + [(1, *p) for p in sent]
    places = [
        (edge, k, row, n * block)
        for k, (edge, row, left, _) in enumerate(pieces)
        for n in range(left.shape[0] // block)
    ]
    blocks = len(places)

    def kernel(marks_ref, cross_ref, norms_ref, other_ref, *refs):
        ins = refs[: 2 * len(pieces)]
        out_ref, high_ref, low_ref = refs[2 * len(pieces) : 2 * len(pieces) + 3]
        power_refs, inverse_refs = refs[-10:-8], refs[-8:-6]
        data_ref, turned_ref, own_high, own_low, in_sems, out_sems = refs[-6:]
        for i, (_, k, _, begin) in enumerate(places):
            for side in range(2):
                load = pltpu.make_async_copy(
                    ins[2 * k + side].at[pl.ds(begin, block), :],
                    data_ref.at[i, :, pl.ds(side * cols, cols)],
                    in_sems.at[2 * i + side],
                )
                load.start()
        edges = []
        for edge in range(2):
            cross = cross_ref[:, edge * per : (edge + 1) * per, :].reshape(cols, cols)
            sign = jnp.where(marks_ref[2 * edge] != 0, 1.0, -1.0).astype(F32)
            edges.append((cross, (norms_ref, other_ref)[edge][...], sign))
        matrices = ((own_high, own_low), (high_ref, low_ref))
        for edge, turns in enumerate(cayley(edges, rows_all, power_refs, inverse_refs)):
            moved_role = marks_ref[2 * edge + 1] != 0
            for half in range(2):
                value = jnp.where(moved_role, turns[2 * half], turns[2 * half + 1])
                store_halves(*matrices[edge], half * cols, 0, value)
        columns = [
            pl.multiple_of(marks_ref[4] * cols, cols),
            pl.multiple_of((1 - marks_ref[4]) * cols, cols),
        ]
        counts = [sum(1 for p in places if p[0] == edge) for edge in range(2)]
        sent_rows = [row + begin for edge, _, row, begin in places if edge]
        apart = sent_rows[1] - sent_rows[0]

        def store_of(i, row, edge):
            return pltpu.make_async_copy(
                turned_ref.at[i],
                out_ref.at[pl.ds(pl.multiple_of(row, block), block), pl.ds(columns[edge], cols)],
                out_sems.at[i],
            )

        def turn(i, row, edge):
            for side in range(2):
                pltpu.make_async_copy(
                    ins[0].at[pl.ds(0, block), :],
                    data_ref.at[i, :, pl.ds(side * cols, cols)],
                    in_sems.at[2 * i + side],
                ).wait()
            x_high, x_low = halves(data_ref[i])
            m_high, m_low = matrices[edge]
            turned_ref[i] = product(x_high, m_high[...]) + (
                product(x_high, m_low[...]) + product(x_low, m_high[...])
            )
            store_of(i, row, edge).start()

        def received_turn(i, carry):
            turn(i, i * block, 0)
            return carry

        def sent_turn(i, carry):
            turn(counts[0] + i, sent_rows[0] + i * apart, 1)
            return carry

        lax.fori_loop(0, counts[0], received_turn, 0)
        lax.fori_loop(0, counts[1], sent_turn, 0)
        for i, (edge, _, row, begin) in enumerate(places):
            store_of(i, row + begin, edge).wait()

    out = jax.ShapeDtypeStruct((2 * cols, cols), BF16)
    vmem = pl.BlockSpec(memory_space=pltpu.VMEM)
    anywhere = pl.BlockSpec(memory_space=pl.ANY)
    return pl.pallas_call(
        kernel,
        in_specs=[
            pl.BlockSpec(memory_space=pltpu.SMEM),
            vmem,
            vmem,
            vmem,
            *[anywhere] * (2 * len(pieces)),
        ],
        out_specs=(anywhere, vmem, vmem),
        out_shape=(jax.ShapeDtypeStruct((rows, 2 * cols), F32), out, out),
        scratch_shapes=[
            *[pltpu.VMEM((cols, cols), F32)] * 4,
            pltpu.VMEM((blocks, block, 2 * cols), F32),
            pltpu.VMEM((blocks, block, cols), F32),
            pltpu.VMEM((2 * cols, cols), BF16),
            pltpu.VMEM((2 * cols, cols), BF16),
            pltpu.SemaphoreType.DMA((2 * blocks,)),
            pltpu.SemaphoreType.DMA((blocks,)),
        ],
        name="step_two",
    )(marks, gathered, norms, other_norms, *[x for p in pieces for x in p[2:]])


def rotate(both, high, low, part, start, rows, block=512):
    width = both.shape[1]
    cols = width // 2

    def kernel(x_ref, high_ref, low_ref, out_ref):
        x_high, x_low = halves(x_ref[...])
        out_ref[...] = product(x_high, high_ref[...]) + (
            product(x_high, low_ref[...]) + product(x_low, high_ref[...])
        )

    at = start // block
    fixed = pl.BlockSpec((width, cols), lambda i: (0, part))
    return pl.pallas_call(
        kernel,
        grid=(rows // block,),
        in_specs=[pl.BlockSpec((block, width), lambda i: (i + at, 0)), fixed, fixed],
        out_specs=pl.BlockSpec((block, cols), lambda i: (i, 0)),
        out_shape=jax.ShapeDtypeStruct((rows, cols), F32),
        name="rotate",
    )(both, high, low)


def combine(at, lefts, rights, high, low, start, rows, before=None, block=512):
    cols = lefts[0].shape[1]
    steps = [x.shape[0] // block for x in lefts]
    begins = [sum(steps[:k]) for k in range(len(steps))]
    pieces, first = len(steps), start // block

    def kernel(at_ref, *refs):
        high_ref, low_ref, out_ref = refs[2 * pieces], refs[2 * pieces + 1], refs[-1]
        step = pl.program_id(0)
        for k in range(pieces):

            @pl.when((step >= begins[k]) & (step < begins[k] + steps[k]))
            def _(k=k):
                total = None
                for line, ref in enumerate((refs[k], refs[pieces + k])):
                    x_high, x_low = halves(ref[...])
                    m_high = high_ref[line * cols : (line + 1) * cols, :]
                    m_low = low_ref[line * cols : (line + 1) * cols, :]
                    part = product(x_high, m_high) + (
                        product(x_high, m_low) + product(x_low, m_high)
                    )
                    total = part if total is None else total + part
                out_ref[...] = total

    data = [
        pl.BlockSpec((block, cols), lambda i, at_ref, b=b, n=n: (jnp.clip(i - b, 0, n - 1), 0))
        for b, n in zip(begins, steps)
    ]
    fixed = pl.BlockSpec((2 * cols, cols), lambda i, at_ref: (0, 0))
    operands = [at, *lefts, *rights, high, low]
    in_specs = [*data, *data, fixed, fixed]
    aliases = {}
    if before is not None:
        operands.append(before)
        in_specs.append(pl.BlockSpec(memory_space=pl.ANY))
        aliases = {len(operands) - 1: 0}
    return pl.pallas_call(
        kernel,
        grid_spec=pltpu.PrefetchScalarGridSpec(
            num_scalar_prefetch=1,
            grid=(sum(steps),),
            in_specs=in_specs,
            out_specs=pl.BlockSpec((block, cols), lambda i, at_ref: (i + first, at_ref[0])),
        ),
        out_shape=jax.ShapeDtypeStruct((rows, 2 * cols), F32),
        input_output_aliases=aliases,
        name="combine",
    )(*operands)


def exchanged(blocks, groups=None):
    return lax.all_to_all(blocks, "rows", 0, 0, axis_index_groups=groups, tiled=True)


def held(value, *until):
    return lax.optimization_barrier((value, *until))[0]


def shards(matrix):
    cols = matrix.shape[1] // 2
    rows = matrix.shape[0]
    peers = lax.axis_size("rows")
    rows_all = rows * peers
    per = cols // peers
    position = lax.axis_index("pairs")
    size = lax.axis_size("pairs")
    ring = [*range(0, size, 2), *range(size - 1, 0, -2)]
    clockwise = [(ring[i], ring[(i + 1) % size]) for i in range(size)]
    back = [(b, a) for a, b in clockwise]
    even = position % 2 == 0
    pieces = [(0, rows // 4), (rows // 4, rows // 2), (3 * rows // 4, rows // 4)]

    slabs = exchanged(gram(matrix, 0, matrix, 1, rows, peers, cols, block=rows // 2))
    spread, norms = slab_sum(slabs, cols, True)
    gathered = exchanged(spread)
    swap = jnp.where(even & (position > 0), 0, 1).astype(jnp.int32)[None]
    high, low, turned = step_one_matrices(
        gathered, norms, swap, matrix, pieces[0][1], float(rows_all)
    )
    onward, arrived = [turned], []
    for k, piece in enumerate(pieces):
        if k:
            onward.append(rotate(matrix, high, low, 0, *piece))
        arrived.append(lax.ppermute(onward[k], "pairs", clockwise))
    kept = [rotate(matrix, high, low, 1, *piece) for piece in pieces]

    line = peers // 2
    halves_of_rows = [[*range(line)], [*range(line, peers)]]
    across = [(i, (i + line) % peers) for i in range(peers)]
    both_ways = [(r * size + b, q * size + a) for r, q in across for b, a in back]
    per = cols // line
    begun = ()
    for k in range(2):
        begun = gram_parts(arrived[k : k + 1], kept[k : k + 1], cols, begun)
    slabs = gram(arrived[2], 0, kept[2], 0, pieces[2][1], line, cols, begun)
    returned = [None] * 3
    returned[0] = lax.ppermute(held(kept[0], slabs), "pairs", back)
    slabs = exchanged(slabs, halves_of_rows)
    mine, _ = slab_sum(slabs, cols, False)
    other = lax.ppermute(mine, "pairs", back)
    partner = lax.ppermute(mine, "rows", across)
    far = lax.ppermute(mine, ("rows", "pairs"), both_ways)
    for at in (2, 1):
        returned[at] = lax.ppermute(held(kept[at], far, partner, other), "pairs", back)
    pair, norms, other_norms = paired(mine, partner, other, far, line, per)
    gathered = exchanged(pair, halves_of_rows)
    in_second = ~even
    marks = jnp.stack(
        [
            (even & (position > 0)) | (position == size - 1),
            position != 0,
            even,
            position == 1,
            in_second,
        ]
    ).astype(jnp.int32)
    begins = [begin for begin, _ in pieces]
    received = list(zip(begins, arrived, kept))
    sent = [(begins[k], onward[k], returned[k]) for k in (0, 2)]
    done, high, low = step_two(
        gathered, norms, other_norms, marks, received, sent, rows, float(rows_all), BLOCK
    )
    in_first = even.astype(jnp.int32)[None]
    return combine(
        in_first, onward[1:2], returned[1:2], high, low, begins[1], rows, done
    )


def solution(mesh):
    return jax.shard_map(
        shards,
        mesh=mesh,
        in_specs=(P("rows", "pairs"),),
        out_specs=P("rows", "pairs"),
        check_vma=False,
    )
```
